8 devices in a mesh: grp: 1 (over z), pp: 2 (over y), dp: 4 (over x, core).
Axes of the slice: x: 2, y: 2, z: 1, core: 2. Of those that a mesh axis runs over, the one named last changes fastest.
Arguments:
- dy: bfloat16 [2, 2048, 1280], P(('grp', 'pp'), 'dp')
- xs: bfloat16 [2, 2, 2, 2048, 1280], P(('grp', 'pp'), None, None, 'dp')
- hs: bfloat16 [2, 2, 2, 2048, 5120], P(('grp', 'pp'), None, None, 'dp')
- w1: bfloat16 [2, 2, 1280, 5120], P(('grp', 'pp'))
- w2: bfloat16 [2, 2, 5120, 1280], P(('grp', 'pp'))
- acc1: float32 [2, 4, 2, 1280, 5120], P(('grp', 'pp'), 'dp')
- acc2: float32 [2, 4, 2, 5120, 1280], P(('grp', 'pp'), 'dp')
Outputs:
- output 1: float32 [2, 2, 1280, 5120], P(('grp', 'pp'), None, 'dp')
- output 2: float32 [2, 2, 5120, 1280], P(('grp', 'pp'), None, 'dp')
- output 3: bfloat16 [2, 2048, 1280], P(('grp', 'pp'), 'dp')
All inputs are finite; a program needn't handle non-finite values.
Results may differ from the reference program's by a relative error of at most 0.00518973.
Values are sent between devices in bfloat16 or wider.
A program may use at most 1 GiB of HBM per device.

```python
import jax
import jax.numpy as jnp
from jax import lax

STAGES = 2
REPS = 4
LAYERS = 2
TOK = 512
DM = 1280
FF = 5120

TOKENS = TOK * REPS


def gelu_fn(v):
    return jax.nn.gelu(v, approximate=True)


def setup_inputs(seed: int = 0, part: int = 0) -> dict:
    key = jax.random.fold_in(jax.random.key(seed), part)
    ks = jax.random.split(key, 7)
    alpha = (2.0 * STAGES * LAYERS) ** -0.5
    s1 = 0.3 * alpha * (STAGES * TOK) ** 0.5
    s2 = 0.65 * (STAGES * TOK) ** 0.5
    dy = jax.random.normal(ks[0], (STAGES, TOKENS, DM), jnp.float32).astype(jnp.bfloat16)
    xs = jax.random.normal(ks[1], (STAGES, STAGES, LAYERS, TOKENS, DM), jnp.float32).astype(jnp.bfloat16)
    hs = jax.random.normal(ks[2], (STAGES, STAGES, LAYERS, TOKENS, FF), jnp.float32).astype(jnp.bfloat16)
    w1 = (jax.random.normal(ks[3], (STAGES, LAYERS, DM, FF), jnp.float32) * DM ** -0.5).astype(jnp.bfloat16)
    w2 = (jax.random.normal(ks[4], (STAGES, LAYERS, FF, DM), jnp.float32) * (FF ** -0.5 * alpha)).astype(jnp.bfloat16)
    acc1 = jax.random.normal(ks[5], (STAGES, REPS, LAYERS, DM, FF), jnp.float32) * s1
    acc2 = jax.random.normal(ks[6], (STAGES, REPS, LAYERS, FF, DM), jnp.float32) * s2
    return {'dy': dy, 'xs': xs, 'hs': hs, 'w1': w1, 'w2': w2, 'acc1': acc1, 'acc2': acc2}


def layer_back(g, x, h, wa, wb):
    act, act_vjp = jax.vjp(gelu_fn, h.astype(jnp.float32))
    u = jnp.dot(g, wb.T, preferred_element_type=jnp.float32)
    dh = act_vjp(u)[0].astype(jnp.bfloat16)
    gx = (g.astype(jnp.float32) + jnp.dot(dh, wa.T, preferred_element_type=jnp.float32)).astype(jnp.bfloat16)
    ab = act.astype(jnp.bfloat16)
    d1 = jnp.einsum('rtd,rtf->rdf', x.reshape(REPS, TOK, DM).astype(jnp.float32), dh.reshape(REPS, TOK, FF).astype(jnp.float32))
    d2 = jnp.einsum('rtf,rtd->rfd', ab.reshape(REPS, TOK, FF).astype(jnp.float32), g.reshape(REPS, TOK, DM).astype(jnp.float32))
    return gx, d1, d2


def stage_back(g, xk, hk, wa, wb, ga, gb):
    def body(c, inp):
        x, h, a1, a2, s1, s2 = inp
        gx, d1, d2 = layer_back(c, x, h, a1, a2)
        return gx, (s1 + d1, s2 + d2)
    gout, (ga2, gb2) = lax.scan(body, g, (xk, hk, wa, wb, ga, gb), reverse=True)
    return gout, ga2, gb2


def reference(dy, xs, hs, w1, w2, acc1, acc2):
    g1_rows = []
    g2_rows = []
    cots = []
    for s in reversed(range(STAGES)):
        ga = jnp.transpose(acc1[s], (1, 0, 2, 3))
        gb = jnp.transpose(acc2[s], (1, 0, 2, 3))
        incoming = cots + [dy[s]]
        outgoing = []
        for j in range(STAGES - s):
            gout, ga, gb = stage_back(incoming[j], xs[s, j], hs[s, j], w1[s], w2[s], ga, gb)
            outgoing.append(gout)
        cots = outgoing
        g1_rows.append(jnp.sum(ga.astype(jnp.bfloat16).astype(jnp.float32), axis=1) / REPS)
        g2_rows.append(jnp.sum(gb.astype(jnp.bfloat16).astype(jnp.float32), axis=1) / REPS)
    g1 = jnp.stack(g1_rows[::-1])
    g2 = jnp.stack(g2_rows[::-1])
    dx = jnp.stack(cots)
    return g1, g2, dx
```

```python
import jax
import jax.numpy as jnp
from jax import lax
from jax.experimental import pallas as pl
from jax.sharding import PartitionSpec as P


def gelu_fn(v):
    return jax.nn.gelu(v, approximate=True)


def act_of(h):
    return gelu_fn(h.astype(jnp.float32)).astype(jnp.bfloat16)


def reduce_into(buf, parts, k, shape, scale, br, first, count):
    cols = shape[2]
    n = len(parts)
    steps = count // br

    def kern(*refs):
        total = refs[0][...].astype(jnp.float32)
        for r in refs[1:n]:
            total = total + r[...].astype(jnp.float32)
        refs[-1][0] = total * scale

    def block(off):
        return pl.BlockSpec((br, cols), lambda i: (off // br + i, 0))

    in_specs = [block(off) for _, off in parts]
    args = [p for p, _ in parts]
    aliases = {}
    if buf is not None:
        in_specs.append(pl.BlockSpec(memory_space=pl.ANY))
        args.append(buf)
        aliases = {n: 0}
    return pl.pallas_call(
        kern, grid=(steps,), in_specs=in_specs,
        out_specs=pl.BlockSpec((1, br, cols), lambda i: (k, first // br + i, 0)),
        out_shape=jax.ShapeDtypeStruct(shape, jnp.float32),
        input_output_aliases=aliases,
        cost_estimate=pl.CostEstimate(flops=count * cols * n, bytes_accessed=count * cols * (2 * n + 4), transcendentals=0),
    )(*args)


def solution(mesh):
    npp = mesh.shape['pp']
    ndp = mesh.shape['dp']
    assert npp == 2 and ndp == 4
    both = ('pp', 'dp')

    def hop(p, routes, off):
        return lax.ppermute(p, both, [(a * ndp + i, b * ndp + (i ^ off)) for a, b in routes for i in range(ndp)])

    def body(dy, xs, hs, w1, w2, acc1, acc2):
        s = lax.axis_index('pp')
        d = lax.axis_index('dp')
        nk = w1.shape[1]
        acc1, acc2, w1, w2, xs, hs = acc1[0, 0], acc2[0, 0], w1[0], w2[0], xs[0], hs[0]
        n1, n2 = acc1.shape[1] // ndp, acc2.shape[1] // ndp
        nc = n2 // 4
        nd = 3 * n2 // 10
        slot = (npp - 1 - s, jnp.int32(0))
        tok = [jnp.int32(0)]

        def after(*v):
            tok[0] = lax.optimization_barrier((tok[0], *v))[0]

        def saved(arr, i, k, at=0, count=None):
            count = count or arr.shape[3]
            return lax.dynamic_slice(arr, (slot[i] + tok[0], k, 0, at), (1, 1, arr.shape[2], count))[0, 0]

        def add(acc, k, at, lhs, rhs):
            part = lax.dynamic_slice(acc, (k, at, 0), (1, lhs.shape[1], acc.shape[2]))[0]
            return (part + jnp.einsum('tr,tc->rc', lhs, rhs, preferred_element_type=jnp.float32)).astype(jnp.bfloat16)

        def early(off, first, count):
            at = (d ^ off) * n2 + first + tok[0]
            p = add(acc2, 1, at, act_of(saved(hs, 0, 1, at, count)), dy[0])
            after(p)
            return p

        def both2(k, off, first=0, count=None):
            at = (d ^ off) * n2 + first + tok[0]
            lhs = jnp.concatenate([lax.dynamic_slice_in_dim(v, at, count or n2, 1) for v in act[k]], 0)
            p = add(acc2, k, at, lhs, jnp.concatenate([ga[k], gb[k]], 0))
            after(p)
            return p

        def both1(k, off):
            at = (d ^ off) * n1 + tok[0]
            lhs = jnp.concatenate([saved(xs, i, k, at, n1) for i in range(2)], 0)
            p = add(acc1, k, at, lhs, jnp.concatenate([da[k], db[k]], 0))
            after(p)
            return p

        def up(g, i, k):
            _, act_vjp = jax.vjp(gelu_fn, saved(hs, i, k).astype(jnp.float32))
            u = jnp.einsum('td,fd->tf', g, w2[k], preferred_element_type=jnp.float32)
            v = act_vjp(u)[0].astype(jnp.bfloat16)
            after(v)
            return v

        def out(g, dh, k):
            v = (g.astype(jnp.float32) + jnp.einsum('tf,df->td', dh, w1[k], preferred_element_type=jnp.float32)).astype(jnp.bfloat16)
            after(v)
            return v

        def acts(k):
            act[k] = lax.optimization_barrier([act_of(saved(hs, i, k)) for i in range(2)])
            after(act[k][0])

        ga, gb, da, db, act = {1: dy[0]}, {}, {}, {}, {}
        stay, down, rise = [(0, 0), (1, 1)], [(1, 0)], [(0, 1)]
        near, own = {}, {}

        c0 = early(3, 0, nc)
        e2 = early(2, 0, n2)
        c1 = early(3, nc, n2 - nc)
        far12 = [(hop(e2, [(1, 1)], 2), 0)]
        lane = [hop(hop(p, down, 0), rise, 3) for p in (c0, c1)]
        da[1] = up(ga[1], 0, 1)
        far11 = []

        def early1(off):
            at = (d ^ off) * n1 + tok[0]
            p = add(acc1, 1, at, saved(xs, 0, 1, at, n1), da[1])
            after(p)
            far11.append((hop(p, [(1, 1)], off), 0))

        early1(2)
        dh, _ = lax.optimization_barrier((da[1], tok[0]))
        ga[0] = out(ga[1], dh, 1)
        da[0] = up(ga[0], 0, 0)
        gout = out(ga[0], da[0], 0)
        recv = lax.ppermute(gout, 'pp', [(1, 0)])
        acts(1)
        early1(3)

        recv, _ = lax.optimization_barrier((recv, tok[0]))
        gb[1] = recv
        far12.append((hop(both2(1, 2), [(0, 0)], 2), 0))
        t = hop(hop(both2(1, 3, 0, nd), rise, 0), down, 3)
        u = hop(both2(1, 3, nd, n2 - nd), [(0, 0)], 3)
        db[1] = up(gb[1], 1, 1)
        gb[0] = out(gb[1], db[1], 1)
        gave = lax.ppermute(lax.optimization_barrier((gout, tok[0]))[0], 'pp', [(0, 1)])
        acts(0)
        far02 = [(hop(both2(0, off), stay, off), 0) for off in (2, 3)]
        far11.append((hop(both1(1, 2), [(0, 0)], 2), 0))
        far11.append((hop(hop(both1(1, 3), rise, 0), down, 3), 0))
        near[1, 2] = hop(both2(1, 1), stay, 1)
        near[1, 1] = hop(both1(1, 1), stay, 1)
        own[1, 2] = both2(1, 0)
        own[1, 1] = both1(1, 0)
        db[0] = up(gb[0], 1, 0)
        near[0, 2] = hop(both2(0, 1), stay, 1)
        own[0, 2] = both2(0, 0)
        p012 = both1(0, 2)
        p013 = both1(0, 3)
        cut = 3 * n1 // 4
        far012 = hop(p012, stay, 2)
        p013a, p013b = lax.optimization_barrier((p013[:cut], p013[cut:]))
        far013a = hop(p013a, stay, 3)
        far013b = hop(p013b, stay, 3)
        dh, _ = lax.optimization_barrier((db[0], tok[0]))
        g = out(gb[0], dh, 0)
        near[0, 1] = hop(both1(0, 1), stay, 1)
        own[0, 1] = both1(0, 0)
        dx = jnp.where(s == 0, g, gave)
        lane, _ = lax.optimization_barrier((lane, tok[0]))
        far12.append((jnp.concatenate(lane, 0), 0))
        far12.append((jnp.concatenate([t, u], 0), 0))
        sc = 1.0 / ndp
        sh1, sh2 = (nk, n1, acc1.shape[2]), (nk, n2, acc2.shape[2])

        def base(k, w, off=0):
            return [(own[k, w], off), (near[k, w], off)]

        o2 = reduce_into(None, base(1, 2) + far12, 1, sh2, sc, n2 // 5, 0, n2)
        o1 = reduce_into(None, base(1, 1) + far11, 1, sh1, sc, n1 // 5, 0, n1)
        o2 = reduce_into(o2, base(0, 2) + far02, 0, sh2, sc, n2 // 5, 0, n2)
        o1 = reduce_into(o1, base(0, 1) + [(far012, 0), (far013a, 0)], 0, sh1, sc, cut // 5, 0, cut)
        br = (n1 - cut) // 5
        o1 = reduce_into(o1, base(0, 1, cut) + [(far012, cut), (far013b, 0)], 0, sh1, sc, br, cut, n1 - cut)
        return o1[None], o2[None], dx[None]

    spec_row = P(('grp', 'pp'), 'dp', None)
    spec_saved = P(('grp', 'pp'), None, None, 'dp', None)
    spec_w = P(('grp', 'pp'), None, None, None)
    spec_acc = P(('grp', 'pp'), 'dp', None, None, None)
    spec_g = P(('grp', 'pp'), None, 'dp', None)
    return jax.shard_map(body, mesh=mesh, in_specs=(spec_row, spec_saved, spec_saved, spec_w, spec_w, spec_acc, spec_acc), out_specs=(spec_g, spec_g, spec_row), check_vma=False)
```

```python
import jax
import jax.numpy as jnp
from jax import lax
from jax.experimental import pallas as pl
from jax.experimental.pallas import tpu as pltpu
from jax.sharding import PartitionSpec as P


C0 = 0.7978845608028654
C1 = C0 * 0.044715


def gelu_tile(h):
    h = h.astype(jnp.float32)
    return (h * (0.5 + 0.5 * jnp.tanh(h * (C0 + C1 * (h * h))))).astype(jnp.bfloat16)


def nt(lhs, rhs):
    return lax.dot_general(lhs, rhs, (((1,), (1,)), ((), ())), preferred_element_type=jnp.float32)


def tn(lhs, rhs):
    return lax.dot_general(lhs, rhs, (((0,), (0,)), ((), ())), preferred_element_type=jnp.float32)


def layer(slot, g, hs, wb, wa, k, bf=1024):
    toks, dm = g.shape
    ff = wb.shape[1]
    nb = ff // bf

    def kern(p, g_ref, h_ref, wb_ref, wa_ref, dh_ref, o_ref, acc):
        i = pl.program_id(0)
        u = nt(g_ref[...], wb_ref[0])
        h = h_ref[0, 0].astype(jnp.float32)
        h2 = h * h
        t = jnp.tanh(h * (C0 + C1 * h2))
        slope = (0.5 + 0.5 * t) + (0.5 * h) * (1.0 - t * t) * (C0 + 3.0 * C1 * h2)
        dh = (slope * u).astype(jnp.bfloat16)
        dh_ref[...] = dh
        v = nt(dh, wa_ref[0])

        @pl.when(i == 0)
        def _():
            acc[...] = v

        @pl.when(i > 0)
        def _():
            acc[...] += v

        @pl.when(i == nb - 1)
        def _():
            o_ref[...] = (g_ref[...].astype(jnp.float32) + acc[...]).astype(jnp.bfloat16)

    return pl.pallas_call(
        kern,
        grid_spec=pltpu.PrefetchScalarGridSpec(
            num_scalar_prefetch=1, grid=(nb,),
            in_specs=[pl.BlockSpec((toks, dm), lambda i, p: (0, 0)), pl.BlockSpec((1, 1, toks, bf), lambda i, p: (p[0], k, 0, i)),
                      pl.BlockSpec((1, bf, dm), lambda i, p: (k, i, 0)), pl.BlockSpec((1, dm, bf), lambda i, p: (k, 0, i))],
            out_specs=[pl.BlockSpec((toks, bf), lambda i, p: (0, i)), pl.BlockSpec((toks, dm), lambda i, p: (0, 0))],
            scratch_shapes=[pltpu.VMEM((toks, dm), jnp.float32)]),
        out_shape=[jax.ShapeDtypeStruct((toks, ff), jnp.bfloat16), jax.ShapeDtypeStruct((toks, dm), jnp.bfloat16)],
        cost_estimate=pl.CostEstimate(flops=4 * toks * dm * ff, bytes_accessed=4 * dm * ff, transcendentals=toks * ff),
        compiler_params=pltpu.CompilerParams(vmem_limit_bytes=48 << 20),
    )(slot.reshape(1), g, hs, wb, wa)


def grad2(at, slots, acc, k, hs, kb, cots, count, bm=256):
    n = len(cots)
    toks, cols = cots[0].shape

    def kern(*refs):
        acc_ref, o_ref = refs[1 + 2 * n], refs[2 + 2 * n]
        total = acc_ref[0]
        for i in range(n):
            total = total + tn(gelu_tile(refs[1 + i][0, 0]), refs[1 + n + i][...])
        o_ref[...] = total.astype(jnp.bfloat16)

    def hspec(j):
        return pl.BlockSpec((1, 1, toks, bm), lambda i, p: (p[1 + j], kb, 0, p[0] + i))

    sp = jnp.stack([at // bm, *slots]).astype(jnp.int32)
    return pl.pallas_call(
        kern,
        grid_spec=pltpu.PrefetchScalarGridSpec(
            num_scalar_prefetch=1, grid=(count // bm,),
            in_specs=[hspec(j) for j in range(n)] + [pl.BlockSpec((toks, cols), lambda i, p: (0, 0))] * n
            + [pl.BlockSpec((1, bm, cols), lambda i, p: (k, p[0] + i, 0))],
            out_specs=pl.BlockSpec((bm, cols), lambda i, p: (i, 0))),
        out_shape=jax.ShapeDtypeStruct((count, cols), jnp.bfloat16),
        cost_estimate=pl.CostEstimate(flops=2 * count * cols * toks * n, bytes_accessed=6 * count * cols, transcendentals=0),
        compiler_params=pltpu.CompilerParams(vmem_limit_bytes=48 << 20),
    )(sp, *[hs] * n, *cots, acc)


def grad1(q, acc, k, lhs, dhs, first=0, count=None):
    bn = 1024
    n = len(lhs)
    rows, toks = lhs[0].shape
    cols = count or dhs[0].shape[1]
    b0 = first // bn

    def kern(*refs):
        acc_ref, o_ref = refs[1 + 2 * n], refs[2 + 2 * n]
        total = acc_ref[0]
        for i in range(n):
            total = total + jnp.dot(refs[1 + i][...], refs[1 + n + i][...], preferred_element_type=jnp.float32)
        o_ref[...] = total.astype(jnp.bfloat16)

    return pl.pallas_call(
        kern,
        grid_spec=pltpu.PrefetchScalarGridSpec(
            num_scalar_prefetch=1, grid=(cols // bn,),
            in_specs=[pl.BlockSpec((rows, toks), lambda i, p: (0, 0))] * n + [pl.BlockSpec((toks, bn), lambda i, p: (0, b0 + i))] * n
            + [pl.BlockSpec((1, rows, bn), lambda i, p: (k, p[0], b0 + i))],
            out_specs=pl.BlockSpec((rows, bn), lambda i, p: (0, i))),
        out_shape=jax.ShapeDtypeStruct((rows, cols), jnp.bfloat16),
        cost_estimate=pl.CostEstimate(flops=2 * rows * cols * toks * n, bytes_accessed=6 * rows * cols, transcendentals=0),
        compiler_params=pltpu.CompilerParams(vmem_limit_bytes=48 << 20),
    )(q.reshape(1), *lhs, *dhs, acc)


def reduce_into(buf, parts, k, shape, scale, br, first, count):
    cols = shape[2]
    n = len(parts)
    steps = count // br

    def kern(*refs):
        total = refs[0][...].astype(jnp.float32)
        for r in refs[1:n]:
            total = total + r[...].astype(jnp.float32)
        refs[-1][0] = total * scale

    def block(off):
        return pl.BlockSpec((br, cols), lambda i: (off // br + i, 0))

    in_specs = [block(off) for _, off in parts]
    args = [p for p, _ in parts]
    aliases = {}
    if buf is not None:
        in_specs.append(pl.BlockSpec(memory_space=pl.ANY))
        args.append(buf)
        aliases = {n: 0}
    return pl.pallas_call(
        kern, grid=(steps,), in_specs=in_specs,
        out_specs=pl.BlockSpec((1, br, cols), lambda i: (k, first // br + i, 0)),
        out_shape=jax.ShapeDtypeStruct(shape, jnp.float32),
        input_output_aliases=aliases,
        cost_estimate=pl.CostEstimate(flops=count * cols * n, bytes_accessed=count * cols * (2 * n + 4), transcendentals=0),
    )(*args)


def solution(mesh):
    npp = mesh.shape['pp']
    ndp = mesh.shape['dp']
    assert npp == 2 and ndp == 4
    both = ('pp', 'dp')

    def hop(p, routes, off):
        return lax.ppermute(p, both, [(a * ndp + i, b * ndp + (i ^ off)) for a, b in routes for i in range(ndp)])

    def body(dy, xs, hs, w1, w2, acc1, acc2):
        s = lax.axis_index('pp')
        d = lax.axis_index('dp')
        nk = w1.shape[1]
        acc1, acc2, w1, w2, xs, hs = acc1[0, 0], acc2[0, 0], w1[0], w2[0], xs[0], hs[0]
        n1, n2 = acc1.shape[1] // ndp, acc2.shape[1] // ndp
        nc = n2 // 5
        nd = 7 * n2 // 10
        slot = (npp - 1 - s, jnp.int32(0))

        def rows_of(i, k, off, arr):
            return lax.dynamic_slice(arr, (slot[i], k, 0, (d ^ off) * n1), (1, 1, arr.shape[2], n1))[0, 0].T

        def early(off, first, count, bm):
            return grad2((d ^ off) * n2 + first, [slot[0]], acc2, 1, hs, 1, [dy[0]], count, bm)

        def both2(k, off, first=0, count=None, bm=640):
            return grad2((d ^ off) * n2 + first, slot, acc2, k, hs, k, [ga[k], gb[k]], count or n2, bm)

        def both1(k, off):
            return grad1(d ^ off, acc1, k, [rows_of(i, k, off, xlate) for i in range(2)], [da[k], db[k]])

        def back(g, i, k):
            return layer(slot[i], g, hs, w2, w1, k)

        ga, gb, da, db = {1: dy[0]}, {}, {}, {}
        stay, down, rise = [(0, 0), (1, 1)], [(1, 0)], [(0, 1)]
        near, own = {}, {}

        c0 = early(3, 0, nc, nc)
        e2 = early(2, 0, n2, n2 // 2)
        c1 = early(3, nc, 2 * nc, nc)
        c2 = early(3, 3 * nc, 2 * nc, nc)
        far12 = [(hop(e2, [(1, 1)], 2), 0)]

        def detour(p, off):
            return hop(hop(p, down, 0), rise, off)

        lane = [detour(p, 3) for p in (c0, c1, c2)]
        da[1], ga[0] = back(ga[1], 0, 1)
        far11 = []

        def early1(off, arr, first=0, count=None):
            return grad1(d ^ off, acc1, 1, [rows_of(0, 1, off, arr)], [da[1]], first, count)

        side = 3 * acc1.shape[2] // 5
        e112 = [detour(early1(2, xs, side, acc1.shape[2] - side), 2)]
        e112.insert(0, hop(early1(2, xs, 0, side), [(1, 1)], 2))
        da[0], gout = back(ga[0], 0, 0)
        gout, xmid = lax.optimization_barrier((gout, xs))
        recv = lax.ppermute(gout, 'pp', [(1, 0)])
        far11.append((hop(early1(3, xmid), [(1, 1)], 3), 0))
        p = grad2((d ^ 2) * n2, [slot[0]], acc2, 0, hs, 0, [ga[0]], n2, n2 // 2)
        far02 = [(hop(p, [(1, 1)], 2), 0)]

        gb[1], xlate = lax.optimization_barrier((recv, xmid))
        recv = gb[1]
        u = hop(both2(1, 3, nd, n2 - nd, nc // 2), [(0, 0)], 3)
        far12.append((hop(both2(1, 2), [(0, 0)], 2), 0))
        t = hop(hop(both2(1, 3, 0, nd, nc // 2), rise, 0), down, 3)
        db[1], gb[0] = back(gb[1], 1, 1)
        gave = lax.ppermute(gout, 'pp', [(0, 1)])
        far02.append((hop(both2(0, 2), [(0, 0)], 2), 0))
        far02.append((hop(both2(0, 3), stay, 3), 0))
        far11.append((hop(both1(1, 2), [(0, 0)], 2), 0))
        far11.append((hop(hop(both1(1, 3), rise, 0), down, 3), 0))
        near[1, 2] = hop(both2(1, 1), stay, 1)
        near[1, 1] = hop(both1(1, 1), stay, 1)
        own[1, 2] = both2(1, 0)
        own[1, 1] = both1(1, 0)
        db[0], g = back(gb[0], 1, 0)
        near[0, 2] = hop(both2(0, 1), stay, 1)
        own[0, 2] = both2(0, 0)
        p012 = both1(0, 2)
        p013 = both1(0, 3)
        cut = 4 * n1 // 5
        p012a, p012b, p013a, p013b = lax.optimization_barrier((p012[:cut], p012[cut:], p013[:cut], p013[cut:]))
        far012a = hop(p012a, stay, 2)
        far013a = hop(p013a, stay, 3)
        near[0, 1] = hop(both1(0, 1), stay, 1)
        own[0, 1] = both1(0, 0)
        dx = jnp.where(s == 0, g, gave)
        far12.append((jnp.concatenate(lane, 0), 0))
        far12.append((jnp.concatenate([t, u], 0), 0))
        far11.append((jnp.concatenate(e112, 1), 0))
        sc = 1.0 / ndp
        sh1, sh2 = (nk, n1, acc1.shape[2]), (nk, n2, acc2.shape[2])

        def base(k, w, off=0):
            return [(own[k, w], off), (near[k, w], off)]

        o2 = reduce_into(None, base(1, 2) + far12, 1, sh2, sc, n2 // 5, 0, n2)
        o1 = reduce_into(None, base(1, 1) + far11, 1, sh1, sc, n1 // 5, 0, n1)
        o2 = reduce_into(o2, base(0, 2) + far02, 0, sh2, sc, n2 // 5, 0, n2)
        far012a, far013a, p012b, p013b, o1, o2 = lax.optimization_barrier((far012a, far013a, p012b, p013b, o1, o2))
        far012b, far013b = hop(p012b, stay, 2), hop(p013b, stay, 3)
        o1 = reduce_into(o1, base(0, 1) + [(far012a, 0), (far013a, 0)], 0, sh1, sc, cut // 8, 0, cut)
        o1 = reduce_into(o1, base(0, 1, cut) + [(far012b, 0), (far013b, 0)], 0, sh1, sc, 16, cut, n1 - cut)
        return o1[None], o2[None], dx[None]

    spec_row = P(('grp', 'pp'), 'dp', None)
    spec_saved = P(('grp', 'pp'), None, None, 'dp', None)
    spec_w = P(('grp', 'pp'), None, None, None)
    spec_acc = P(('grp', 'pp'), 'dp', None, None, None)
    spec_g = P(('grp', 'pp'), None, 'dp', None)
    return jax.shard_map(body, mesh=mesh, in_specs=(spec_row, spec_saved, spec_saved, spec_w, spec_w, spec_acc, spec_acc), out_specs=(spec_g, spec_g, spec_row), check_vma=False)
```

```python
import jax
import jax.numpy as jnp
from jax import lax
from jax.experimental import pallas as pl
from jax.experimental.pallas import tpu as pltpu
from jax.sharding import PartitionSpec as P


C0 = 0.7978845608028654
C1 = C0 * 0.044715


def gelu_tile(h):
    h = h.astype(jnp.float32)
    return (h * (0.5 + 0.5 * jnp.tanh(h * (C0 + C1 * (h * h))))).astype(jnp.bfloat16)


def nt(lhs, rhs):
    return lax.dot_general(lhs, rhs, (((1,), (1,)), ((), ())), preferred_element_type=jnp.float32)


def tn(lhs, rhs):
    return lax.dot_general(lhs, rhs, (((0,), (0,)), ((), ())), preferred_element_type=jnp.float32)


def layer(slot, g, hs, wb, wa, k, bf=1024):
    toks, dm = g.shape
    ff = wb.shape[1]
    nb = ff // bf

    def kern(p, g_ref, h_ref, wb_ref, wa_ref, dh_ref, o_ref, acc):
        i = pl.program_id(0)
        u = nt(g_ref[...], wb_ref[0])
        h = h_ref[0, 0].astype(jnp.float32)
        h2 = h * h
        t = jnp.tanh(h * (C0 + C1 * h2))
        slope = (0.5 + 0.5 * t) + (0.5 * h) * (1.0 - t * t) * (C0 + 3.0 * C1 * h2)
        dh = (slope * u).astype(jnp.bfloat16)
        dh_ref[...] = dh
        v = nt(dh, wa_ref[0])

        @pl.when(i == 0)
        def _():
            acc[...] = v

        @pl.when(i > 0)
        def _():
            acc[...] += v

        @pl.when(i == nb - 1)
        def _():
            o_ref[...] = (g_ref[...].astype(jnp.float32) + acc[...]).astype(jnp.bfloat16)

    return pl.pallas_call(
        kern,
        grid_spec=pltpu.PrefetchScalarGridSpec(
            num_scalar_prefetch=1, grid=(nb,),
            in_specs=[pl.BlockSpec((toks, dm), lambda i, p: (0, 0)), pl.BlockSpec((1, 1, toks, bf), lambda i, p: (p[0], k, 0, i)),
                      pl.BlockSpec((1, bf, dm), lambda i, p: (k, i, 0)), pl.BlockSpec((1, dm, bf), lambda i, p: (k, 0, i))],
            out_specs=[pl.BlockSpec((toks, bf), lambda i, p: (0, i)), pl.BlockSpec((toks, dm), lambda i, p: (0, 0))],
            scratch_shapes=[pltpu.VMEM((toks, dm), jnp.float32)]),
        out_shape=[jax.ShapeDtypeStruct((toks, ff), jnp.bfloat16), jax.ShapeDtypeStruct((toks, dm), jnp.bfloat16)],
        cost_estimate=pl.CostEstimate(flops=4 * toks * dm * ff, bytes_accessed=4 * dm * ff, transcendentals=toks * ff),
        compiler_params=pltpu.CompilerParams(vmem_limit_bytes=48 << 20),
    )(slot.reshape(1), g, hs, wb, wa)


def grad2(at, slots, acc, k, hs, kb, cots, count, bm=256):
    n = len(cots)
    sub = 256 if n == 1 and bm % 256 == 0 else 128
    assert bm % sub == 0 and count % bm == 0
    toks, cols = cots[0].shape

    def kern(*refs):
        acc_ref, o_ref = refs[1 + 2 * n], refs[2 + 2 * n]

        def part(j, _):
            at = pl.ds(pl.multiple_of(j * sub, sub), sub)
            total = acc_ref[0, at]
            for i in range(n):
                total = total + tn(gelu_tile(refs[1 + i][0, 0, :, at]), refs[1 + n + i][...])
            o_ref[at] = total.astype(jnp.bfloat16)
            return 0

        lax.fori_loop(0, bm // sub, part, 0)

    def hspec(j):
        return pl.BlockSpec((1, 1, toks, bm), lambda i, p: (p[1 + j], kb, 0, p[0] + i))

    sp = jnp.stack([at // bm, *slots]).astype(jnp.int32)
    return pl.pallas_call(
        kern,
        grid_spec=pltpu.PrefetchScalarGridSpec(
            num_scalar_prefetch=1, grid=(count // bm,),
            in_specs=[hspec(j) for j in range(n)] + [pl.BlockSpec((toks, cols), lambda i, p: (0, 0))] * n
            + [pl.BlockSpec((1, bm, cols), lambda i, p: (k, p[0] + i, 0))],
            out_specs=pl.BlockSpec((bm, cols), lambda i, p: (i, 0))),
        out_shape=jax.ShapeDtypeStruct((count, cols), jnp.bfloat16),
        cost_estimate=pl.CostEstimate(flops=2 * count * cols * toks * n, bytes_accessed=6 * count * cols, transcendentals=0),
        compiler_params=pltpu.CompilerParams(vmem_limit_bytes=48 << 20),
    )(sp, *[hs] * n, *cots, acc)


def grad1(q, acc, k, lhs, dhs, first=0, count=None):
    bn = 1024
    n = len(lhs)
    sub = 256 if n == 1 else 128
    rows, toks = lhs[0].shape
    cols = count or dhs[0].shape[1]
    assert cols % bn == 0 and bn % sub == 0 and first % bn == 0
    b0 = first // bn

    def kern(*refs):
        acc_ref, o_ref = refs[1 + 2 * n], refs[2 + 2 * n]

        def part(j, _):
            at = pl.ds(pl.multiple_of(j * sub, sub), sub)
            total = acc_ref[0, :, at]
            for i in range(n):
                total = total + jnp.dot(refs[1 + i][...], refs[1 + n + i][:, at], preferred_element_type=jnp.float32)
            o_ref[:, at] = total.astype(jnp.bfloat16)
            return 0

        lax.fori_loop(0, bn // sub, part, 0)

    return pl.pallas_call(
        kern,
        grid_spec=pltpu.PrefetchScalarGridSpec(
            num_scalar_prefetch=1, grid=(cols // bn,),
            in_specs=[pl.BlockSpec((rows, toks), lambda i, p: (0, 0))] * n + [pl.BlockSpec((toks, bn), lambda i, p: (0, b0 + i))] * n
            + [pl.BlockSpec((1, rows, bn), lambda i, p: (k, p[0], b0 + i))],
            out_specs=pl.BlockSpec((rows, bn), lambda i, p: (0, i))),
        out_shape=jax.ShapeDtypeStruct((rows, cols), jnp.bfloat16),
        cost_estimate=pl.CostEstimate(flops=2 * rows * cols * toks * n, bytes_accessed=6 * rows * cols, transcendentals=0),
        compiler_params=pltpu.CompilerParams(vmem_limit_bytes=48 << 20),
    )(q.reshape(1), *lhs, *dhs, acc)


def reduce_into(buf, parts, k, shape, scale, br, first, count):
    cols = shape[2]
    n = len(parts)
    steps = count // br

    def kern(*refs):
        def some(j, _):
            at = pl.ds(pl.multiple_of(j * 16, 16), 16)
            total = refs[0][at].astype(jnp.float32)
            for r in refs[1:n]:
                total = total + r[at].astype(jnp.float32)
            refs[-1][0, at] = total * scale
            return 0

        lax.fori_loop(0, br // 16, some, 0)

    def block(off):
        return pl.BlockSpec((br, cols), lambda i: (off // br + i, 0))

    in_specs = [block(off) for _, off in parts]
    args = [p for p, _ in parts]
    aliases = {}
    if buf is not None:
        in_specs.append(pl.BlockSpec(memory_space=pl.ANY))
        args.append(buf)
        aliases = {n: 0}
    return pl.pallas_call(
        kern, grid=(steps,), in_specs=in_specs,
        out_specs=pl.BlockSpec((1, br, cols), lambda i: (k, first // br + i, 0)),
        out_shape=jax.ShapeDtypeStruct(shape, jnp.float32),
        input_output_aliases=aliases,
        cost_estimate=pl.CostEstimate(flops=count * cols * n, bytes_accessed=count * cols * (2 * n + 4), transcendentals=0),
    )(*args)


def solution(mesh):
    npp = mesh.shape['pp']
    ndp = mesh.shape['dp']
    assert npp == 2 and ndp == 4
    both = ('pp', 'dp')

    def hop(p, routes, off):
        return lax.ppermute(p, both, [(a * ndp + i, b * ndp + (i ^ off)) for a, b in routes for i in range(ndp)])

    def body(dy, xs, hs, w1, w2, acc1, acc2):
        s = lax.axis_index('pp')
        d = lax.axis_index('dp')
        nk = w1.shape[1]
        acc1, acc2, w1, w2, xs, hs = acc1[0, 0], acc2[0, 0], w1[0], w2[0], xs[0], hs[0]
        n1, n2 = acc1.shape[1] // ndp, acc2.shape[1] // ndp
        nc = n2 // 5
        nd = 7 * n2 // 10
        slot = (npp - 1 - s, jnp.int32(0))

        def rows_of(i, k, off, arr):
            return lax.dynamic_slice(arr, (slot[i], k, 0, (d ^ off) * n1), (1, 1, arr.shape[2], n1))[0, 0].T

        def early(off, first, count, bm):
            return grad2((d ^ off) * n2 + first, [slot[0]], acc2, 1, hs, 1, [dy[0]], count, bm)

        def both2(k, off, first=0, count=None, bm=640):
            return grad2((d ^ off) * n2 + first, slot, acc2, k, hs, k, [ga[k], gb[k]], count or n2, bm)

        def both1(k, off):
            return grad1(d ^ off, acc1, k, [rows_of(i, k, off, xlate) for i in range(2)], [da[k], db[k]])

        def back(g, i, k):
            return layer(slot[i], g, hs, w2, w1, k, 512)

        ga, gb, da, db = {1: dy[0]}, {}, {}, {}
        stay, down, rise = [(0, 0), (1, 1)], [(1, 0)], [(0, 1)]
        near, own = {}, {}

        c0 = early(3, 0, nc, nc)
        e2 = early(2, 0, n2, n2 // 2)
        c1 = early(3, nc, 2 * nc, nc)
        c2 = early(3, 3 * nc, 2 * nc, nc)
        far12 = [(hop(e2, [(1, 1)], 2), 0)]

        def detour(p, off):
            return hop(hop(p, down, 0), rise, off)

        lane = [detour(p, 3) for p in (c0, c1, c2)]
        da[1], ga[0] = back(ga[1], 0, 1)
        far11 = []

        def early1(off, arr, first=0, count=None):
            return grad1(d ^ off, acc1, 1, [rows_of(0, 1, off, arr)], [da[1]], first, count)

        side = 3 * acc1.shape[2] // 5
        e112 = [detour(early1(2, xs, side, acc1.shape[2] - side), 2)]
        e112.insert(0, hop(early1(2, xs, 0, side), [(1, 1)], 2))
        da[0], gout = back(ga[0], 0, 0)
        gout, xmid = lax.optimization_barrier((gout, xs))
        recv = lax.ppermute(gout, 'pp', [(1, 0)])
        far11.append((hop(early1(3, xmid), [(1, 1)], 3), 0))
        p = grad2((d ^ 2) * n2, [slot[0]], acc2, 0, hs, 0, [ga[0]], n2, n2 // 2)
        far02 = [(hop(p, [(1, 1)], 2), 0)]

        gb[1], xlate = lax.optimization_barrier((recv, xmid))
        recv = gb[1]
        u = hop(both2(1, 3, nd, n2 - nd, nc // 2), [(0, 0)], 3)
        far12.append((hop(both2(1, 2), [(0, 0)], 2), 0))
        t = hop(hop(both2(1, 3, 0, nd, nc // 2), rise, 0), down, 3)
        db[1], gb[0] = back(gb[1], 1, 1)
        gave = lax.ppermute(gout, 'pp', [(0, 1)])
        far02.append((hop(both2(0, 2), [(0, 0)], 2), 0))
        far02.append((hop(both2(0, 3), stay, 3), 0))
        far11.append((hop(both1(1, 2), [(0, 0)], 2), 0))
        far11.append((hop(hop(both1(1, 3), rise, 0), down, 3), 0))
        near[1, 2] = hop(both2(1, 1), stay, 1)
        near[1, 1] = hop(both1(1, 1), stay, 1)
        own[1, 2] = both2(1, 0)
        own[1, 1] = both1(1, 0)
        db[0], g = back(gb[0], 1, 0)
        near[0, 2] = hop(both2(0, 1), stay, 1)
        own[0, 2] = both2(0, 0)
        p012 = both1(0, 2)
        p013 = both1(0, 3)
        cut = 4 * n1 // 5
        p012a, p012b, p013a, p013b = lax.optimization_barrier((p012[:cut], p012[cut:], p013[:cut], p013[cut:]))
        far012a = hop(p012a, stay, 2)
        far013a = hop(p013a, stay, 3)
        near[0, 1] = hop(both1(0, 1), stay, 1)
        own[0, 1] = both1(0, 0)
        dx = jnp.where(s == 0, g, gave)
        far12.append((jnp.concatenate(lane, 0), 0))
        far12.append((jnp.concatenate([t, u], 0), 0))
        far11.append((jnp.concatenate(e112, 1), 0))
        sc = 1.0 / ndp
        sh1, sh2 = (nk, n1, acc1.shape[2]), (nk, n2, acc2.shape[2])

        def base(k, w, off=0):
            return [(own[k, w], off), (near[k, w], off)]

        o2 = reduce_into(None, base(1, 2) + far12, 1, sh2, sc, n2 // 5, 0, n2)
        o1 = reduce_into(None, base(1, 1) + far11, 1, sh1, sc, n1 // 5, 0, n1)
        o2 = reduce_into(o2, base(0, 2) + far02, 0, sh2, sc, n2 // 5, 0, n2)
        far012a, far013a, p012b, p013b, o1, o2 = lax.optimization_barrier((far012a, far013a, p012b, p013b, o1, o2))
        far012b, far013b = hop(p012b, stay, 2), hop(p013b, stay, 3)
        o1 = reduce_into(o1, base(0, 1) + [(far012a, 0), (far013a, 0)], 0, sh1, sc, cut // 4, 0, cut)
        o1 = reduce_into(o1, base(0, 1, cut) + [(far012b, 0), (far013b, 0)], 0, sh1, sc, 16, cut, n1 - cut)
        return o1[None], o2[None], dx[None]

    spec_row = P(('grp', 'pp'), 'dp', None)
    spec_saved = P(('grp', 'pp'), None, None, 'dp', None)
    spec_w = P(('grp', 'pp'), None, None, None)
    spec_acc = P(('grp', 'pp'), 'dp', None, None, None)
    spec_g = P(('grp', 'pp'), None, 'dp', None)
    return jax.shard_map(body, mesh=mesh, in_specs=(spec_row, spec_saved, spec_saved, spec_w, spec_w, spec_acc, spec_acc), out_specs=(spec_g, spec_g, spec_row), check_vma=False)
```
